256 devices in a mesh: row: 16 (over z_lo, x), col: 16 (over z_hi, y, core).
Axes of the slice: x: 4, y: 4, z: 8 (z_hi: 2, z_lo: 4; z = z_hi * 4 + z_lo), core: 2. Of those that a mesh axis runs over, the one named last changes fastest.
Arguments:
- samples: float32 [32768, 512], P(('row', 'col')), may hold values from -8 to 8
- labels: int32 [32768, 256], P(('row', 'col')), may hold values from -1 to 1, as said below
Outputs:
- statistic: float32 [256], replicated
- proof: float32 [32768], P(('row', 'col'))
- p_value: float32 [], replicated
The draws below stay inside these ranges and needn't reach their ends.
Inputs may be any that keep to these rules, and one draw needn't show every extreme that they name: `labels`: every column holds exactly 16384 entries +1 and 16384 entries -1.
All inputs are finite; a program needn't handle non-finite values.
Results may differ from the reference program's by a relative error of at most 0.0003.
Values sent between devices are 32-bit elements; how exact they have to be, the bound alone decides.
No kernel may reach another device: no remote copies, remote signals or barrier semaphores. Data moves between devices by JAX's collectives and lax.ppermute only.
A program may use at most 64 MiB of HBM per device.

```python
import math
import jax
import jax.numpy as jnp
from jax import lax

W = 512
PERMS = 256
NS = 32768


def draw_samples(key, part):
    base = jax.random.fold_in(key, 11)
    member_key, center_key, spread_key, jitter_key, scale_key = jax.random.split(base, 5)
    member = jax.random.randint(member_key, (NS,), 0, 128)
    spread = jnp.exp(jax.random.uniform(spread_key, (128, 1), jnp.float32, jnp.log(0.7), jnp.log(2.5)))
    scales = jnp.exp(jax.random.uniform(scale_key, (NS, 1), jnp.float32, jnp.log(0.25), jnp.log(1.0)))
    centers = jnp.clip(jax.random.normal(center_key, (128, W), jnp.float32), -2.5, 2.5)
    jitter = jnp.clip(jax.random.normal(jitter_key, (NS, W), jnp.float32), -1.5, 1.5)
    placed = (centers * spread)[member]
    return (placed + jitter * scales).astype(jnp.float32)


def draw_labels(key, part):
    keys = jax.random.split(jax.random.fold_in(key, 23), PERMS)
    orders = jax.vmap(lambda one: jax.random.permutation(one, NS))(keys)
    return jnp.where(orders < NS // 2, 1, -1).astype(jnp.int32).T


def setup_inputs(seed: int = 0) -> dict:
    key_list = jax.random.split(jax.random.key(seed), 3)
    return {
        "samples": draw_samples(jax.random.fold_in(key_list[2], 71), 0),
        "labels": draw_labels(jax.random.fold_in(key_list[2], 71), 0),
    }


def tile_terms(xr, lr, gr, xc, lc, gc, width):
    norm_rows = lax.optimization_barrier(jnp.sum(xr * xr, 1))
    norm_cols = lax.optimization_barrier(jnp.sum(xc * xc, 1))
    dots = lax.dot_general(xr, xc, (((1,), (1,)), ((), ())), precision=lax.Precision.HIGHEST, preferred_element_type=jnp.float32)
    dist = jnp.maximum(norm_rows[:, None] + norm_cols[None, :] - 2.0 * dots, 0.0)
    kern = jnp.where(gr[:, None] == gc[None, :], 0.0, jnp.exp(-dist / (2.0 * width)))
    proj = jnp.dot(kern, lc, precision=lax.Precision.HIGHEST, preferred_element_type=jnp.float32)
    return (proj[:, 0], lax.optimization_barrier(jnp.sum(lr * proj, 0)), jnp.sum(kern))

def reference(samples, labels):
    total_rows = samples.shape[0]
    width = samples.shape[1]
    perms = labels.shape[1]
    labs = labels.astype(jnp.float32)
    tile = math.gcd(total_rows, 1024)
    count = total_rows // tile
    ids = jnp.arange(total_rows, dtype=jnp.int32)

    def one(args):
        xr, lr, gr = args
        return tile_terms(xr, lr, gr, samples, labs, ids, width)
    wit, quad, tot = lax.map(one, (samples.reshape(count, tile, width), labs.reshape(count, tile, perms), ids.reshape(count, tile)))
    quad = lax.optimization_barrier(jnp.sum(quad, 0))
    total = jnp.sum(tot)
    half = total_rows / 2.0
    statistic = total / (2.0 * half * (half - 1.0)) + (2.0 * half - 1.0) / (2.0 * half * (half - 1.0)) * quad
    proof = wit.reshape(total_rows) / jnp.sqrt(jnp.float32(total_rows))
    p_value = jnp.mean(jax.nn.sigmoid(4.0 * (statistic[1:] - statistic[0])))
    return (statistic, proof, p_value)
```

```python
import functools

import jax
import jax.numpy as jnp
from jax import lax
from jax.experimental import pallas as pl
from jax.experimental.pallas import tpu as pltpu
from jax.sharding import Mesh
from jax.sharding import PartitionSpec as P

AXES = ("zl", "x", "zh", "y", "c")
SIZES = (4, 4, 2, 4, 2)
BLK = 128
W = 512
PERMS = 256
COLS = W + PERMS
F32 = jnp.float32
BF16 = jnp.bfloat16

SELF = ((0, 0), (2, 0), (0, 2), (2, 2))
FULL = ((1, 0), (0, 3), (1, 1), (1, 3), (3, 2), (2, 1))


def index(zl, x, zh, y, c):
    return (((zl * 4 + x) * 2 + zh) * 4 + y) * 2 + c


def pairs(dx, dy, dz, dc):
    out = []
    for zl in range(4):
        for x in range(4):
            for zh in range(2):
                for y in range(4):
                    for c in range(2):
                        z = (zh * 4 + zl + dz) % 8
                        src = index(z % 4, (x + dx) % 4, z // 4, (y + dy) % 4, (c + dc) % 2)
                        out.append((src, index(zl, x, zh, y, c)))
    return out


def take(v, name, dx=0, dy=0, dz=0, dc=0):
    with jax.named_scope(name):
        return lax.ppermute(v, AXES, pairs(dx, dy, dz, dc))


def pack_kernel(s_ref, l_ref, o_ref):
    o_ref[:, :W] = s_ref[...]
    o_ref[:, W:] = l_ref[...].astype(F32)


def halves(x):
    hi = x.astype(BF16)
    return hi, (x - hi.astype(F32)).astype(BF16)


def spread_norm(x):
    n = jnp.sum(x * x, axis=1, keepdims=True) * (0.5 / W)
    return jnp.broadcast_to(n, (BLK, 128))


def pair_kernel(tiles, chunks, n_r, n_c, *refs):
    r_refs = refs[:n_r]
    c_refs = refs[n_r : n_r + n_c]
    out = refs[n_r + n_c]
    rs, cs, lc, ar, lr, bc, acc, wc, tt = refs[n_r + n_c + 1 :]
    for j, ref in enumerate(c_refs):
        x = ref[:, :W]
        hi, lo = halves(x)
        rows = slice(j * BLK, (j + 1) * BLK)
        cs[rows, :W] = hi
        cs[rows, W : 2 * W] = lo
        cs[rows, 2 * W :] = hi
        lc[rows, :] = ref[:, W:].astype(BF16)
        bc[:, rows] = spread_norm(x).T[:8, :]
    for i, ref in enumerate(r_refs):
        x = ref[:, :W]
        hi, lo = halves(x * (1.0 / W))
        rows = slice(i * BLK, (i + 1) * BLK)
        rs[rows, :W] = hi
        rs[rows, W : 2 * W] = hi
        rs[rows, 2 * W :] = lo
        ar[rows, :] = spread_norm(x)
        lr[rows, :] = jnp.broadcast_to(ref[:, W : W + 1], (BLK, 128))
    acc[...] = jnp.zeros_like(acc)
    wc[...] = jnp.zeros_like(wc)
    tt[...] = jnp.zeros_like(tt)

    def piece(t, start, width, weight, diag):
        rows = pl.ds(t * 256, 256) if isinstance(t, int) else pl.ds(pl.multiple_of(t * 256, 256), 256)
        cols = slice(start, start + width)
        s = lax.dot_general(rs[rows, :], cs[cols, :], (((1,), (1,)), ((), ())), preferred_element_type=F32)
        a = ar[rows, :]
        lrow = lr[rows, :]
        if width > 128:
            a = jnp.concatenate([a] * (width // 128), axis=1)
            lrow = jnp.concatenate([lrow] * (width // 128), axis=1)
        k = jnp.exp(jnp.minimum((s - a) - bc[0:1, cols], 0.0))
        if weight != 1.0:
            k = k * weight
        if diag:
            i = lax.broadcasted_iota(jnp.int32, k.shape, 0)
            j = lax.broadcasted_iota(jnp.int32, k.shape, 1)
            k = jnp.where((i == j) & (i < BLK), 0.0, k)
        hi, lo = halves(k)
        lab = lc[cols, :]
        acc[rows, :] += jnp.dot(hi, lab, preferred_element_type=F32) + jnp.dot(lo, lab, preferred_element_type=F32)
        wc[0:1, cols] += jnp.sum(k * lrow, axis=0, keepdims=True)
        tt[0:1, cols] += jnp.sum(k, axis=0, keepdims=True)

    start = 0
    for blocks, kind in chunks:
        width = blocks * BLK
        if kind == "full":

            def body(t, carry, start=start, width=width):
                piece(t, start, width, 1.0, False)
                return carry

            lax.fori_loop(0, len(tiles), body, 0)
        else:
            for t, dz in enumerate(tiles):
                if dz in (0, 4):
                    piece(t, start, width, 0.5, dz == 0 and kind == "own")
                elif dz < 4:
                    piece(t, start, width, 1.0, False)
        start += width

    quad = jnp.zeros((1, PERMS), F32)
    for i, ref in enumerate(r_refs):
        rows = slice(i * BLK, (i + 1) * BLK)
        part = acc[rows, :]
        quad = quad + jnp.sum(part * ref[:, W:], axis=0, keepdims=True)
        out[i : i + 1, :] = part[:, :128].T[0:1, :]
    tot = jnp.zeros((1, 128), F32)
    for j in range(n_c):
        cols = slice(j * BLK, (j + 1) * BLK)
        out[n_r + j : n_r + j + 1, :] = wc[0:1, cols]
        tot = tot + tt[0:1, cols]
    out[n_r + n_c : n_r + n_c + 1, :] = quad[:, :128]
    out[n_r + n_c + 1 : n_r + n_c + 2, :] = quad[:, 128:]
    out[n_r + n_c + 2 : n_r + n_c + 3, :] = tot


def pair_call(rows, columns, name):
    tiles = [dz for dz, _, _ in rows]
    r_in = [b for _, own, other in rows for b in (own, other)]
    chunks = [(len(blocks), kind) for blocks, kind in columns]
    c_in = [b for blocks, _ in columns for b in blocks]
    n_r, n_c = len(r_in), len(c_in)
    n_out = -(-(n_r + n_c + 3) // 8) * 8
    cells = sum(
        256 * b * BLK * (len(tiles) if kind == "full" else sum(dz <= 4 for dz in tiles)) for b, kind in chunks
    )
    vmem = pl.BlockSpec(memory_space=pltpu.VMEM)
    out = pl.pallas_call(
        functools.partial(pair_kernel, tiles, chunks, n_r, n_c),
        out_shape=jax.ShapeDtypeStruct((n_out, 128), F32),
        in_specs=[vmem] * (n_r + n_c),
        out_specs=vmem,
        scratch_shapes=[
            pltpu.VMEM((n_r * BLK, 3 * W), BF16),
            pltpu.VMEM((n_c * BLK, 3 * W), BF16),
            pltpu.VMEM((n_c * BLK, PERMS), BF16),
            pltpu.VMEM((n_r * BLK, 128), F32),
            pltpu.VMEM((n_r * BLK, 128), F32),
            pltpu.VMEM((8, n_c * BLK), F32),
            pltpu.VMEM((n_r * BLK, PERMS), F32),
            pltpu.VMEM((8, n_c * BLK), F32),
            pltpu.VMEM((8, n_c * BLK), F32),
        ],
        cost_estimate=pl.CostEstimate(
            flops=cells * 2 * (3 * W + 2 * PERMS), bytes_accessed=(n_r + n_c) * BLK * COLS * 4, transcendentals=cells
        ),
        name=name,
    )(*r_in, *c_in)
    return out[:n_r], out[n_r : n_r + n_c], out[n_r + n_c : n_r + n_c + 2].reshape(PERMS), out[n_r + n_c + 2]


def shards(samples, labels):
    vmem = pl.BlockSpec(memory_space=pltpu.VMEM)
    own = pl.pallas_call(
        pack_kernel,
        out_shape=jax.ShapeDtypeStruct((BLK, COLS), F32),
        in_specs=[vmem, vmem],
        out_specs=vmem,
        name="pack",
    )(samples, labels)
    c02 = take(own, "c02", dy=2)
    c20 = take(own, "c20", dx=2)
    u1 = take(own, "u1", dz=1)
    d1 = take(own, "d1", dz=-1)
    c10 = take(own, "c10", dx=1)
    c03 = take(own, "c03", dy=-1)
    o0 = take(own, "o0", dc=1)
    u2 = take(u1, "u2", dz=1)
    d2 = take(d1, "d2", dz=-1)
    c21 = take(c20, "c21", dy=1)
    c22 = take(c02, "c22", dx=2)
    c32 = take(c02, "c32", dx=-1)
    c11 = take(c10, "c11", dy=1)
    c13 = take(c10, "c13", dy=-1)
    u3 = take(u2, "u3", dz=1)
    d3 = take(d2, "d3", dz=-1)
    u4 = take(u3, "u4", dz=1)
    near = [(dz, b, take(b, f"o{dz}", dc=1)) for dz, b in ((1, u1), (7, d1), (2, u2), (6, d2))]
    mid = [(dz, b, take(b, f"o{dz}", dc=1)) for dz, b in ((3, u3), (5, d3))]
    last = [(4, u4, take(u4, "o4", dc=1))]
    near = [(0, own, o0)] + near
    first = [([c10, c03], "full"), ([own, c20], "own"), ([c02], "self")]
    second = [([c11, c13], "full"), ([c32, c21], "full"), ([c22], "self")]
    first_at = [(1, 0), (0, 3), (0, 0), (2, 0), (0, 2)]
    second_at = [(1, 1), (1, 3), (3, 2), (2, 1), (2, 2)]

    at = {a: lax.axis_index(a) for a in AXES}
    z = at["zh"] * 4 + at["zl"]
    peer = jnp.arange(256, dtype=jnp.int32)
    peer_c, peer_y, peer_x = peer % 2, peer // 2 % 4, peer // 16 % 4
    peer_z = peer // 8 % 2 * 4 + peer // 64

    def place(rows, here):
        return jnp.where(here[:, None], rows[None, :], 0.0)

    wit = jnp.zeros((256, BLK), F32)
    quad = jnp.zeros((PERMS,), F32)
    total = jnp.zeros((BLK,), F32)
    row_sums, col_sums = {}, {}
    for rows, columns, where, name in (
        (near, first, first_at, "near_first"),
        (near, second, second_at, "near_second"),
        (mid, first + second, first_at + second_at, "mid_all"),
        (last, first + second, first_at + second_at, "last_all"),
    ):
        r, c, q, t = pair_call(rows, columns, name)
        quad = quad + q
        total = total + t
        for i, (dz, _, _) in enumerate(rows):
            for side in range(2):
                key = (dz, side)
                row_sums[key] = row_sums.get(key, 0.0) + r[2 * i + side]
        for j, key in enumerate(where):
            col_sums[key] = col_sums.get(key, 0.0) + c[j]
    line = (peer_x == at["x"]) & (peer_y == at["y"])
    for (dz, side), v in row_sums.items():
        wit = wit + place(v, line & (peer_z == (z + dz) % 8) & (peer_c == (at["c"] + side) % 2))
    plane = (peer_z == z) & (peer_c == at["c"])
    for (dx, dy), v in col_sums.items():
        wit = wit + place(v, plane & (peer_x == (at["x"] + dx) % 4) & (peer_y == (at["y"] + dy) % 4))

    all_rows = samples.shape[0] * 256
    half = all_rows / 2.0
    share = 2.0 * jnp.sum(total) / (2.0 * half * (half - 1.0)) + (2.0 * half - 1.0) / (2.0 * half * (half - 1.0)) * (
        2.0 * quad
    )
    sent = jnp.concatenate([wit, jnp.broadcast_to(share[None, :], (256, PERMS))], axis=1)
    with jax.named_scope("meet"):
        got = jnp.sum(lax.all_to_all(sent, AXES, 0, 0, tiled=True), axis=0)
    proof = got[:BLK] / jnp.sqrt(jnp.float32(all_rows))
    statistic = got[BLK:]
    p_value = jnp.mean(jax.nn.sigmoid(4.0 * (statistic[1:] - statistic[0])))
    return (statistic, proof, p_value)


def solution(mesh):
    torus = Mesh(mesh.devices.reshape(SIZES), AXES)
    return jax.shard_map(
        shards,
        mesh=torus,
        in_specs=(P(AXES, None), P(AXES, None)),
        out_specs=(P(), P(AXES), P()),
        check_vma=False,
    )
```

```python
import functools

import jax
import jax.numpy as jnp
from jax import lax
from jax.experimental import pallas as pl
from jax.experimental.pallas import tpu as pltpu
from jax.sharding import Mesh
from jax.sharding import PartitionSpec as P


AXES = ("zl", "x", "zh", "y", "c")
SIZES = (4, 4, 2, 4, 2)
BLK = 128
W = 512
PERMS = 256
COLS = W + PERMS
F32 = jnp.float32
BF16 = jnp.bfloat16

FIRST = ((0, 0), (2, 0), (0, 2), (1, 0), (0, 3))
SECOND = ((1, 1), (1, 3), (3, 2), (2, 1))
THIRD = ((2, 2),)
SELF = {"first": 3, "second": 0, "third": 1}
COUNT = {"first": 5, "second": 4, "third": 1}
NEAR = (0, 1, 2, 7, 6)
MID = (3, 5)
LAST = (4,)


def index(zl, x, zh, y, c):
    return (((zl * 4 + x) * 2 + zh) * 4 + y) * 2 + c


def pairs(dx, dy, dz, dc):
    out = []
    for zl in range(4):
        for x in range(4):
            for zh in range(2):
                for y in range(4):
                    for c in range(2):
                        z = (zh * 4 + zl + dz) % 8
                        src = index(z % 4, (x + dx) % 4, z // 4, (y + dy) % 4, (c + dc) % 2)
                        out.append((src, index(zl, x, zh, y, c)))
    return out


def take(v, dx=0, dy=0, dz=0, dc=0):
    return lax.ppermute(v, AXES, pairs(dx, dy, dz, dc))


def pack_kernel(s_ref, l_ref, o_ref):
    o_ref[:, :W] = s_ref[...]
    o_ref[:, W:] = l_ref[...].astype(F32)


def halves(x):
    hi = x.astype(BF16)
    return hi, (x - hi.astype(F32)).astype(BF16)


def spread_norm(x):
    n = jnp.sum(x * x, axis=1, keepdims=True) * (0.5 / W)
    return jnp.broadcast_to(n, (BLK, 128))


class Rows:
    def __init__(self, tiles):
        n = 2 * len(tiles) * BLK
        self.tiles = tiles
        self.shapes = [((n, 2 * W + PERMS), BF16), ((n, 128), F32)]

    def fill(self, refs, raw):
        for i, ref in enumerate(raw):
            rows = slice(i * BLK, (i + 1) * BLK)
            x = ref[:, :W]
            hi, lo = halves(x * (1.0 / W))
            refs[0][rows, :W] = hi
            refs[0][rows, W : 2 * W] = lo
            refs[0][rows, 2 * W :] = ref[:, W:].astype(BF16)
            refs[1][rows, :] = spread_norm(x)


class Columns:
    def __init__(self, name):
        n = COUNT[name] * BLK
        self.width = n
        self.own = SELF[name] * BLK
        self.diag = name == "first"
        self.shapes = [((n, 2 * W + PERMS), BF16), ((8, n), F32)]

    def fill(self, refs, raw):
        for j, ref in enumerate(raw):
            rows = slice(j * BLK, (j + 1) * BLK)
            x = ref[:, :W]
            hi, lo = halves(x)
            refs[0][rows, :W] = lo
            refs[0][rows, W : 2 * W] = hi
            refs[0][rows, 2 * W :] = ref[:, W:].astype(BF16)
            refs[1][:, rows] = spread_norm(x).T[:8, :]


def dot_nt(a, b):
    return lax.dot_general(a, b, (((1,), (1,)), ((), ())), preferred_element_type=F32)


def side_by_side(a, width):
    return jnp.concatenate([a] * (width // 128), axis=1)


def piece(rows, r, cols, c, first, count, acc, wc, tt):
    dz = rows.tiles[first]
    lanes = slice(0 if dz <= 4 else cols.own, cols.width)
    width = lanes.stop - lanes.start
    at = slice(first * 256, (first + count) * 256)
    s = dot_nt(r[0][at, : 2 * W], c[0][lanes, : 2 * W]) + dot_nt(r[0][at, :W], c[0][lanes, W : 2 * W])
    s = (s - side_by_side(r[1][at, :], width)) - c[1][0:1, lanes]
    k = jnp.exp(jnp.minimum(s, 0.0))
    if dz in (0, 4) and cols.own == width:
        k = k * 0.5
    elif dz in (0, 4) and cols.own:
        lane = lax.broadcasted_iota(jnp.int32, (1, width), 1)
        k = k * jnp.where(lane < cols.own, 0.5, 1.0)
    if dz == 0 and cols.diag:
        i = lax.broadcasted_iota(jnp.int32, (BLK, BLK), 0)
        j = lax.broadcasted_iota(jnp.int32, (BLK, BLK), 1)
        top = jnp.concatenate([jnp.where(i == j, 0.0, k[:BLK, :BLK]), k[:BLK, BLK:]], axis=1)
        k = jnp.concatenate([top, k[BLK:, :]], axis=0)
    hi, lo = halves(k)
    lab = c[0][lanes, 2 * W :]
    acc[at, :] += jnp.dot(hi, lab, preferred_element_type=F32) + jnp.dot(lo, lab, preferred_element_type=F32)
    observed = jnp.broadcast_to(r[0][at, 2 * W : 2 * W + 1].astype(F32), (count * 256, 128))
    wc[0:1, lanes] += jnp.sum(k * side_by_side(observed, width), axis=0, keepdims=True)
    tt[0:1, lanes] += jnp.sum(k, axis=0, keepdims=True)


def groups(tiles):
    out = []
    for t, dz in enumerate(tiles):
        kind = 0 if dz in (0, 4) else 1 if dz < 4 else 2
        if out and out[-1][2] == kind and out[-1][1] < 2:
            out[-1][1] += 1
        else:
            out.append([t, 1, kind])
    return [(first, count) for first, count, _ in out]


def sums_of(rows, r, accs, out, base, count=None):
    quad = jnp.zeros((1, PERMS), F32)
    for i in range(count or 2 * len(rows.tiles)):
        at = slice(i * BLK, (i + 1) * BLK)
        part = accs[at, :]
        quad = quad + jnp.sum(part * r[0][at, 2 * W :].astype(F32), axis=0, keepdims=True)
        out[base + i : base + i + 1, :] = part[:, :128].T[0:1, :]
    return quad


def cell_shapes(n_rows, *names):
    sums = [((8, COUNT[name] * BLK), F32) for name in names for _ in range(2)]
    return [((n, PERMS), F32) for n in n_rows] + sums


def finish(out, base, quad, column_sums, totals):
    tot = jnp.zeros((1, 128), F32)
    for wc, tt in zip(column_sums, totals):
        for j in range(wc.shape[1] // BLK):
            cols = slice(j * BLK, (j + 1) * BLK)
            out[base : base + 1, :] = wc[0:1, cols]
            tot = tot + tt[0:1, cols]
            base += 1
    out[base : base + 1, :] = quad[:, :128]
    out[base + 1 : base + 2, :] = quad[:, 128:]
    out[base + 2 : base + 3, :] = tot


def clear(*refs):
    for ref in refs:
        ref[...] = jnp.zeros_like(ref)


def kernel_one(*refs):
    rows, cols = Rows(NEAR), Columns("first")
    raw_r, raw_c, out, r, c, (acc, wc, tt) = cut(refs, 10, 5, 1, 2, 2, 3)
    rows.fill(r, raw_r)
    cols.fill(c, raw_c)
    clear(acc, wc, tt)
    for first, count in groups(NEAR):
        piece(rows, r, cols, c, first, count, acc, wc, tt)
    quad = sums_of(rows, r, acc, out[0], 0)
    finish(out[0], 10, quad, [wc], [tt])


def kernel_two(*refs):
    near, mid, one, two = Rows(NEAR), Rows(MID), Columns("first"), Columns("second")
    raw_r, raw_c, rn, c1, out, c2, rm, (an, am, w1, t1, w2, t2) = cut(refs, 4, 4, 2, 2, 1, 2, 2, 6)
    mid.fill(rm, raw_r)
    two.fill(c2, raw_c)
    clear(an, am, w1, t1, w2, t2)
    for first, count in groups(NEAR):
        piece(near, rn, two, c2, first, count, an, w2, t2)
    for first, count in groups(MID):
        piece(mid, rm, one, c1, first, count, am, w1, t1)
        piece(mid, rm, two, c2, first, count, am, w2, t2)
    quad = sums_of(near, rn, an, out[0], 0) + sums_of(mid, rm, am, out[0], 10)
    finish(out[0], 14, quad, [w1, w2], [t1, t2])


def kernel_three(all_rows, *refs):
    near, mid, last = Rows(NEAR), Rows(MID), Rows(LAST)
    one, two, three = Columns("first"), Columns("second"), Columns("third")
    raw_r, raw_c, rn, rm, c1, c2, (p1, p2), sent, rl, c3, (an, am, al, *sums, p3) = cut(
        refs, 2, 1, 2, 2, 2, 2, 2, 1, 2, 2, 10
    )
    w1, t1, w2, t2, w3, t3 = sums
    last.fill(rl, raw_r)
    three.fill(c3, raw_c)
    clear(an, am, al, *sums)
    for first, count in groups(NEAR):
        if NEAR[first] <= 4:
            piece(near, rn, three, c3, first, count, an, w3, t3)
    piece(mid, rm, three, c3, 0, 1, am, w3, t3)
    piece(last, rl, one, c1, 0, 1, al, w1, t1)
    piece(last, rl, two, c2, 0, 1, al, w2, t2)
    piece(last, rl, three, c3, 0, 1, al, w3, t3)
    quad = sums_of(near, rn, an, p3, 0, 6) + sums_of(mid, rm, am, p3, 6, 2) + sums_of(last, rl, al, p3, 8)
    finish(p3, 10, quad, [w1, w2, w3], [t1, t2, t3])

    half = all_rows / 2.0
    pair = 2.0 * half * (half - 1.0)
    total = jnp.sum(p1[17:18, :] + p2[25:26, :] + p3[22:23, :])
    sent = sent[0]
    for k in range(2):
        q = p1[15 + k : 16 + k, :] + p2[23 + k : 24 + k, :] + p3[20 + k : 21 + k, :]
        share = (2.0 / pair) * total + (2.0 * (2.0 * half - 1.0) / pair) * q
        sent[:, (1 + k) * BLK : (2 + k) * BLK] = jnp.broadcast_to(share, (256, BLK))
    zl, x, zh, y, c = (lax.axis_index(a) for a in AXES)
    z = zh * 4 + zl
    device = lax.broadcasted_iota(jnp.int32, (256, BLK), 0)
    wit = jnp.zeros((256, BLK), F32)
    for side in range(2):
        for i, dz in enumerate(NEAR + MID + LAST):
            j = 2 * i + side
            if j == 0:
                continue
            if dz in NEAR:
                v = p1[j : j + 1, :] + p2[j : j + 1, :]
            elif dz in MID:
                v = p2[j : j + 1, :]
            else:
                v = p3[8 + side : 9 + side, :]
            if j < 6:
                v = v + p3[j : j + 1, :]
            if dz == 3:
                v = v + p3[6 + side : 7 + side, :]
            pz = (z + dz) % 8
            peer = index(pz % 4, x, pz // 4, y, (c + side) % 2)
            wit = jnp.where(device == peer, v, wit)
    for i, (dx, dy) in enumerate(FIRST + SECOND + THIRD):
        v = p3[10 + i : 11 + i, :]
        if i < 9:
            v = v + p2[14 + i : 15 + i, :]
        if i < 5:
            v = v + p1[10 + i : 11 + i, :]
        if i == 0:
            v = v + p1[0:1, :] + p2[0:1, :] + p3[0:1, :]
        peer = index(zl, (x + dx) % 4, zh, (y + dy) % 4, c)
        wit = jnp.where(device == peer, v, wit)
    sent[:, :BLK] = wit


def kernel_end(all_rows, got, statistic, proof, p_value):
    both = jnp.sum(got[...], axis=0)
    proof[...] = both[:, :BLK] / jnp.sqrt(jnp.full((1, BLK), all_rows, F32))
    s = both[:, BLK:]
    statistic[...] = s
    part = jax.nn.sigmoid(4.0 * (s - s[:, 0:1]))
    lane = lax.broadcasted_iota(jnp.int32, (1, PERMS), 1)
    p_value[...] = jnp.sum(jnp.where(lane > 0, part, 0.0), axis=1, keepdims=True) / (PERMS - 1.0)


def cut(refs, *lengths):
    out, start = [], 0
    for n in lengths:
        out.append(refs[start : start + n])
        start += n
    return out


def pair_call(body, ins, outs, scratch, cells):
    vmem = pl.BlockSpec(memory_space=pltpu.VMEM)
    return pl.pallas_call(
        body,
        out_shape=[jax.ShapeDtypeStruct(*s) for s in outs],
        in_specs=[vmem] * len(ins),
        out_specs=[vmem] * len(outs),
        scratch_shapes=[pltpu.VMEM(*s) for s in scratch],
        cost_estimate=pl.CostEstimate(
            flops=int(cells * 131072) * (3 * W + 2 * PERMS), bytes_accessed=8 << 20, transcendentals=int(cells * 65536)
        ),
        compiler_params=pltpu.CompilerParams(vmem_limit_bytes=8 << 20),
    )(*ins)


def shards(samples, labels):
    vmem = pl.BlockSpec(memory_space=pltpu.VMEM)
    all_rows = samples.shape[0] * 256
    own = pl.pallas_call(
        pack_kernel,
        out_shape=jax.ShapeDtypeStruct((BLK, COLS), F32),
        in_specs=[vmem, vmem],
        out_specs=vmem,
        compiler_params=pltpu.CompilerParams(vmem_limit_bytes=4 << 20),
        name="pack",
    )(samples, labels)
    u1 = take(own, dz=1)
    d1 = take(own, dz=-1)
    c10 = take(own, dx=1)
    c03 = take(own, dy=-1)
    c20 = take(c10, dx=1)
    c02 = take(c03, dy=-1)
    u2 = take(u1, dz=1)
    d2 = take(d1, dz=-1)
    c32 = take(c02, dx=-1)
    c22 = take(c32, dx=-1)
    c21 = take(c20, dy=1)
    c11 = take(c10, dy=1)
    c13 = take(c10, dy=-1)
    u3 = take(u2, dz=1)
    d3 = take(d2, dz=-1)
    u4 = take(u3, dz=1)
    line = {0: own, 1: u1, 2: u2, 3: u3, 4: u4, 5: d3, 6: d2, 7: d1}
    rows = {dz: (b, take(b, dc=1)) for dz, b in line.items()}

    def raw(tiles):
        return [b for dz in tiles for b in rows[dz]]

    near, mid, last = Rows(NEAR), Rows(MID), Rows(LAST)
    one, two, three = Columns("first"), Columns("second"), Columns("third")
    p1, *ready = pair_call(
        kernel_one,
        [*raw(NEAR), own, c20, c02, c10, c03],
        [((24, 128), F32), *near.shapes, *one.shapes],
        cell_shapes((1280,), "first"),
        9.5,
    )
    rn, c1 = ready[:2], ready[2:]
    p2, *ready = pair_call(
        kernel_two,
        [*raw(MID), c11, c13, c32, c21, *rn, *c1],
        [((32, 128), F32), *two.shapes, *mid.shapes],
        cell_shapes((1280, 512), "first", "second"),
        17.5,
    )
    c2, rm = ready[:2], ready[2:]
    (sent,) = pair_call(
        functools.partial(kernel_three, all_rows),
        [*raw(LAST), c22, *rn, *rm, *c1, *c2, p1, p2],
        [((256, COLS // 2), F32)],
        [
            *last.shapes,
            *three.shapes,
            *cell_shapes((1280, 512, 256), "first", "second", "third"),
            ((24, 128), F32),
        ],
        7.0,
    )
    got = lax.all_to_all(sent.reshape(256, 1, COLS // 2), AXES, 0, 0, tiled=True)
    statistic, proof, p_value = pl.pallas_call(
        functools.partial(kernel_end, float(all_rows)),
        out_shape=[jax.ShapeDtypeStruct((1, n), F32) for n in (PERMS, BLK, 1)],
        in_specs=[vmem],
        out_specs=[vmem] * 3,
        compiler_params=pltpu.CompilerParams(vmem_limit_bytes=8 << 20),
        name="end",
    )(got)
    return (statistic.reshape(PERMS), proof.reshape(BLK), p_value.reshape(()))


def solution(mesh):
    torus = Mesh(mesh.devices.reshape(SIZES), AXES)
    return jax.shard_map(
        shards,
        mesh=torus,
        in_specs=(P(AXES, None), P(AXES, None)),
        out_specs=(P(), P(AXES), P()),
        check_vma=False,
    )
```

```python
import functools

import jax
import jax.numpy as jnp
from jax import lax
from jax.experimental import pallas as pl
from jax.experimental.pallas import tpu as pltpu
from jax.sharding import Mesh
from jax.sharding import PartitionSpec as P


AXES = ("zl", "x", "zh", "y", "c")
SIZES = (4, 4, 2, 4, 2)
BLK = 128
W = 512
PERMS = 256
COLS = W + PERMS
F32 = jnp.float32
BF16 = jnp.bfloat16

ROWS = {"near": (0, 1, 7), "next": (2, 6), "mid": (3, 5), "last": (4,)}
COLUMNS = {
    "a": ((0, 0), (1, 0), (0, 3)),
    "b": ((2, 0), (0, 2)),
    "c": ((1, 1), (1, 3), (3, 2), (2, 1)),
    "d": ((2, 2),),
}
SELF = {"a": 1, "b": 2, "c": 0, "d": 1}

JOBS = {
    "k0": (("near", "a"),),
    "k1": (("near", "b"), ("next", "a"), ("next", "b")),
    "k2": (("near", "c"), ("next", "c"), ("mid", "a"), ("mid", "b"), ("mid", "c")),
    "k3": (("near", "d"), ("next", "d"), ("mid", "d")),
    "k4": (("last", "a"), ("last", "b"), ("last", "c"), ("last", "d")),
}


def index(zl, x, zh, y, c):
    return (((zl * 4 + x) * 2 + zh) * 4 + y) * 2 + c


def pairs(dx, dy, dz, dc):
    out = []
    for zl in range(4):
        for x in range(4):
            for zh in range(2):
                for y in range(4):
                    for c in range(2):
                        z = (zh * 4 + zl + dz) % 8
                        src = index(z % 4, (x + dx) % 4, z // 4, (y + dy) % 4, (c + dc) % 2)
                        out.append((src, index(zl, x, zh, y, c)))
    return out


def take(v, dx=0, dy=0, dz=0, dc=0):
    return lax.ppermute(v, AXES, pairs(dx, dy, dz, dc))


def pack_kernel(s_ref, l_ref, o_ref):
    o_ref[:, :W] = s_ref[...]
    o_ref[:, W:] = l_ref[...].astype(F32)


def halves(x):
    hi = x.astype(BF16)
    return hi, (x - hi.astype(F32)).astype(BF16)


def spread_norm(x):
    n = jnp.sum(x * x, axis=1, keepdims=True) * (0.5 / W)
    return jnp.broadcast_to(n, (BLK, 128))


class Rows:
    def __init__(self, name):
        self.tiles = ROWS[name]
        self.blocks = 2 * len(self.tiles)
        n = self.blocks * BLK
        self.shapes = [((n, 2 * W + PERMS), BF16), ((n, 128), F32)]
        self.sums = [((n, PERMS), F32)]

    def fill(self, refs, raw):
        for i, ref in enumerate(raw):
            rows = slice(i * BLK, (i + 1) * BLK)
            x = ref[:, :W]
            hi, lo = halves(x * (1.0 / W))
            refs[0][rows, :W] = hi
            refs[0][rows, W : 2 * W] = lo
            refs[0][rows, 2 * W :] = ref[:, W:].astype(BF16)
            refs[1][rows, :] = spread_norm(x)


class Columns:
    def __init__(self, name):
        self.blocks = len(COLUMNS[name])
        self.width = self.blocks * BLK
        self.own = SELF[name] * BLK
        self.diag = COLUMNS[name][0] == (0, 0)
        self.shapes = [((self.width, 2 * W + PERMS), BF16), ((8, self.width), F32)]
        self.sums = [((8, self.width), F32)] * 2

    def fill(self, refs, raw):
        for j, ref in enumerate(raw):
            rows = slice(j * BLK, (j + 1) * BLK)
            x = ref[:, :W]
            hi, lo = halves(x)
            refs[0][rows, :W] = lo
            refs[0][rows, W : 2 * W] = hi
            refs[0][rows, 2 * W :] = ref[:, W:].astype(BF16)
            refs[1][:, rows] = spread_norm(x).T[:8, :]


def first_use(name):
    return next(job for job, work in JOBS.items() if any(name in pair for pair in work))


def sets_of(job):
    rows = list(dict.fromkeys(r for r, _ in JOBS[job]))
    cols = list(dict.fromkeys(c for _, c in JOBS[job]))
    return rows, cols


def sum_rows(job):
    at, start = {}, 0
    rows, cols = sets_of(job)
    for name in (*rows, *cols):
        at[name] = start
        start += Rows(name).blocks if name in ROWS else Columns(name).blocks
    return {**at, "end": start}


def dot_nt(a, b):
    return lax.dot_general(a, b, (((1,), (1,)), ((), ())), preferred_element_type=F32)


def side_by_side(a, width):
    return jnp.concatenate([a] * (width // 128), axis=1)


def piece(rows, r, cols, c, first, count, acc, wc, tt):
    dz = rows.tiles[first]
    lanes = slice(0 if dz <= 4 else cols.own, cols.width)
    width = lanes.stop - lanes.start
    at = slice(first * 256, (first + count) * 256)
    s = dot_nt(r[0][at, : 2 * W], c[0][lanes, : 2 * W]) + dot_nt(r[0][at, :W], c[0][lanes, W : 2 * W])
    s = (s - side_by_side(r[1][at, :], width)) - c[1][0:1, lanes]
    k = jnp.exp(jnp.minimum(s, 0.0))
    if dz in (0, 4) and cols.own == width:
        k = k * 0.5
    elif dz in (0, 4) and cols.own:
        lane = lax.broadcasted_iota(jnp.int32, (1, width), 1)
        k = k * jnp.where(lane < cols.own, 0.5, 1.0)
    if dz == 0 and cols.diag:
        i = lax.broadcasted_iota(jnp.int32, (BLK, BLK), 0)
        j = lax.broadcasted_iota(jnp.int32, (BLK, BLK), 1)
        top = jnp.concatenate([jnp.where(i == j, 0.0, k[:BLK, :BLK]), k[:BLK, BLK:]], axis=1)
        k = jnp.concatenate([top, k[BLK:, :]], axis=0)
    hi, lo = halves(k)
    lab = c[0][lanes, 2 * W :]
    acc[at, :] += jnp.dot(hi, lab, preferred_element_type=F32) + jnp.dot(lo, lab, preferred_element_type=F32)
    observed = jnp.broadcast_to(r[0][at, 2 * W : 2 * W + 1].astype(F32), (count * 256, 128))
    wc[0:1, lanes] += jnp.sum(k * side_by_side(observed, width), axis=0, keepdims=True)
    tt[0:1, lanes] += jnp.sum(k, axis=0, keepdims=True)


def groups(rows, cols):
    out = []
    for t, dz in enumerate(rows.tiles):
        kind = 1 if not cols.own else 0 if dz in (0, 4) else 1 if dz < 4 else 2
        if kind == 2 and cols.own == cols.width:
            continue
        if out and out[-1][2] == kind and out[-1][0] + out[-1][1] == t and out[-1][1] < 3:
            out[-1][1] += 1
        else:
            out.append([t, 1, kind])
    return [(first, count) for first, count, _ in out]


def clear(*refs):
    for ref in refs:
        ref[...] = jnp.zeros_like(ref)


def job_kernel(job, raw_counts, ready_names, made_names, tail, *refs):
    rows, cols = sets_of(job)
    shape_of = {name: Rows(name) if name in ROWS else Columns(name) for name in (*rows, *cols)}
    refs = list(refs)

    def pop(n):
        head, refs[:] = refs[:n], refs[n:]
        return head

    raw = {name: pop(n) for name, n in raw_counts}
    ready = {name: pop(2) for name in ready_names}
    before = pop(tail)
    out = pop(1)[0]
    made = {name: pop(2) for name in made_names}
    for name, _ in raw_counts:
        ready[name] = made[name] if name in made else pop(2)
        shape_of[name].fill(ready[name], raw[name])
    acc = {name: pop(1)[0] for name in rows}
    sums = {name: pop(2) for name in cols}
    if tail:
        sent, out = out, pop(1)[0]
    clear(*acc.values(), *(ref for pair in sums.values() for ref in pair))
    for r, c in JOBS[job]:
        for first, count in groups(shape_of[r], shape_of[c]):
            piece(shape_of[r], ready[r], shape_of[c], ready[c], first, count, acc[r], *sums[c])
    at = sum_rows(job)
    quad = jnp.zeros((1, PERMS), F32)
    for name in rows:
        for i in range(shape_of[name].blocks):
            here = slice(i * BLK, (i + 1) * BLK)
            part = acc[name][here, :]
            quad = quad + jnp.sum(part * ready[name][0][here, 2 * W :].astype(F32), axis=0, keepdims=True)
            out[at[name] + i : at[name] + i + 1, :] = part[:, :128].T[0:1, :]
    tot = jnp.zeros((1, 128), F32)
    for name in cols:
        wc, tt = sums[name]
        for j in range(shape_of[name].blocks):
            lanes = slice(j * BLK, (j + 1) * BLK)
            out[at[name] + j : at[name] + j + 1, :] = wc[0:1, lanes]
            tot = tot + tt[0:1, lanes]
    end = at["end"]
    out[end : end + 1, :] = quad[:, :128]
    out[end + 1 : end + 2, :] = quad[:, 128:]
    out[end + 2 : end + 3, :] = tot
    if tail:
        send_sums(tuple(zip(JOBS, [*before, out])), sent)


def send_sums(parts, sent):
    def row_of(name, i):
        found = [(ref, sum_rows(job)) for job, ref in parts]
        rows = [ref[at[name] + i : at[name] + i + 1, :] for ref, at in found if name in at]
        return functools.reduce(jnp.add, rows)

    all_rows = 256 * BLK
    half = all_rows / 2.0
    pair = 2.0 * half * (half - 1.0)
    total = jnp.sum(row_of("end", 2))
    for k in range(2):
        share = (2.0 / pair) * total + (2.0 * (2.0 * half - 1.0) / pair) * row_of("end", k)
        sent[:, (1 + k) * BLK : (2 + k) * BLK] = jnp.broadcast_to(share, (256, BLK))
    zl, x, zh, y, c = (lax.axis_index(a) for a in AXES)
    z = zh * 4 + zl
    device = lax.broadcasted_iota(jnp.int32, (256, BLK), 0)
    wit = jnp.zeros((256, BLK), F32)
    for name, tiles in ROWS.items():
        for i, dz in enumerate(tiles):
            for side in range(2):
                if dz == 0 and side == 0:
                    continue
                pz = (z + dz) % 8
                peer = index(pz % 4, x, pz // 4, y, (c + side) % 2)
                wit = jnp.where(device == peer, row_of(name, 2 * i + side), wit)
    for name, offsets in COLUMNS.items():
        for i, (dx, dy) in enumerate(offsets):
            v = row_of(name, i)
            if (dx, dy) == (0, 0):
                v = v + row_of("near", 0)
            peer = index(zl, (x + dx) % 4, zh, (y + dy) % 4, c)
            wit = jnp.where(device == peer, v, wit)
    sent[:, :BLK] = wit


def kernel_end(all_rows, got, statistic, proof, p_value):
    both = jnp.sum(got[...], axis=0)
    proof[...] = both[:, :BLK] / jnp.sqrt(jnp.full((1, BLK), all_rows, F32))
    s = both[:, BLK:]
    statistic[...] = s
    part = jax.nn.sigmoid(4.0 * (s - s[:, 0:1]))
    lane = lax.broadcasted_iota(jnp.int32, (1, PERMS), 1)
    p_value[...] = jnp.sum(jnp.where(lane > 0, part, 0.0), axis=1, keepdims=True) / (PERMS - 1.0)


def run(job, raw, ready, before=None):
    rows, cols = sets_of(job)
    names = [name for name in (*rows, *cols) if first_use(name) == job]
    reused = [name for name in (*rows, *cols) if first_use(name) != job]
    shape_of = {name: Rows(name) if name in ROWS else Columns(name) for name in (*rows, *cols)}
    made = [] if before else names
    ins = [b for name in names for b in raw[name]] + [a for name in reused for a in ready[name]] + (before or [])
    n_out = -(-(sum_rows(job)["end"] + 3) // 8) * 8
    outs = [((256, 1 * BLK + PERMS), F32) if before else ((n_out, 128), F32)]
    outs += [s for name in made for s in shape_of[name].shapes]
    scratch = [s for name in names if name not in made for s in shape_of[name].shapes]
    scratch += [s for name in (*rows, *cols) for s in shape_of[name].sums]
    if before:
        scratch.append(((n_out, 128), F32))
    cells = sum(Rows(r).blocks * Columns(c).blocks for r, c in JOBS[job]) * BLK * BLK
    vmem = pl.BlockSpec(memory_space=pltpu.VMEM)
    out, *bundles = pl.pallas_call(
        functools.partial(job_kernel, job, [(name, len(raw[name])) for name in names], reused, made, len(before or [])),
        out_shape=[jax.ShapeDtypeStruct(*s) for s in outs],
        in_specs=[vmem] * len(ins),
        out_specs=[vmem] * len(outs),
        scratch_shapes=[pltpu.VMEM(*s) for s in scratch],
        cost_estimate=pl.CostEstimate(
            flops=cells * 2 * (3 * W + 2 * PERMS), bytes_accessed=8 << 20, transcendentals=cells
        ),
        compiler_params=pltpu.CompilerParams(vmem_limit_bytes=8 << 20),
    )(*ins)
    for k, name in enumerate(made):
        ready[name] = bundles[2 * k : 2 * k + 2]
    return out


def shards(samples, labels):
    vmem = pl.BlockSpec(memory_space=pltpu.VMEM)
    all_rows = samples.shape[0] * 256
    own = pl.pallas_call(
        pack_kernel,
        out_shape=jax.ShapeDtypeStruct((BLK, COLS), F32),
        in_specs=[vmem, vmem],
        out_specs=vmem,
        compiler_params=pltpu.CompilerParams(vmem_limit_bytes=4 << 20),
        name="pack",
    )(samples, labels)
    u1 = take(own, dz=1)
    d1 = take(own, dz=-1)
    c10 = take(own, dx=1)
    c03 = take(own, dy=-1)
    c20 = take(c10, dx=1)
    c02 = take(c03, dy=-1)
    u2 = take(u1, dz=1)
    d2 = take(d1, dz=-1)
    c32 = take(c02, dx=-1)
    c22 = take(c32, dx=-1)
    c21 = take(c20, dy=1)
    c11 = take(c10, dy=1)
    c13 = take(c10, dy=-1)
    u3 = take(u2, dz=1)
    d3 = take(d2, dz=-1)
    u4 = take(u3, dz=1)
    line = {0: own, 1: u1, 2: u2, 3: u3, 4: u4, 5: d3, 6: d2, 7: d1}
    rows = {dz: (b, take(b, dc=1)) for dz, b in line.items()}

    plane = {
        **{(0, 0): own, (1, 0): c10, (0, 3): c03, (2, 0): c20, (0, 2): c02},
        **{(1, 1): c11, (1, 3): c13, (3, 2): c32, (2, 1): c21, (2, 2): c22},
    }
    raw = {name: [b for dz in tiles for b in rows[dz]] for name, tiles in ROWS.items()}
    raw |= {name: [plane[at] for at in offsets] for name, offsets in COLUMNS.items()}
    ready, before = {}, []
    for job in list(JOBS)[:-1]:
        before.append(run(job, raw, ready))
    sent = run(list(JOBS)[-1], raw, ready, before)
    got = lax.all_to_all(sent.reshape(256, 1, COLS // 2), AXES, 0, 0, tiled=True)
    statistic, proof, p_value = pl.pallas_call(
        functools.partial(kernel_end, float(all_rows)),
        out_shape=[jax.ShapeDtypeStruct((1, n), F32) for n in (PERMS, BLK, 1)],
        in_specs=[vmem],
        out_specs=[vmem] * 3,
        compiler_params=pltpu.CompilerParams(vmem_limit_bytes=8 << 20),
        name="end",
    )(got)
    return (statistic.reshape(PERMS), proof.reshape(BLK), p_value.reshape(()))


def solution(mesh):
    torus = Mesh(mesh.devices.reshape(SIZES), AXES)
    return jax.shard_map(
        shards,
        mesh=torus,
        in_specs=(P(AXES, None), P(AXES, None)),
        out_specs=(P(), P(AXES), P()),
        check_vma=False,
    )
```

```python
import functools

import jax
import jax.numpy as jnp
from jax import lax
from jax.experimental import pallas as pl
from jax.experimental.pallas import tpu as pltpu
from jax.sharding import Mesh
from jax.sharding import PartitionSpec as P


AXES = ("zl", "x", "zh", "y", "c")
SIZES = (4, 4, 2, 4, 2)
BLK = 128
W = 512
PERMS = 256
COLS = W + PERMS
F32 = jnp.float32
BF16 = jnp.bfloat16

ROWS = {"near": (0, 1, 7), "next": (2, 6), "mid": (3, 5), "last": (4,)}
COLUMNS = {
    "a": ((0, 0), (1, 0), (0, 3)),
    "b": ((2, 0), (0, 2)),
    "c": ((1, 1), (1, 3), (3, 2), (2, 1)),
    "d": ((2, 2),),
}
SELF = {"a": 1, "b": 2, "c": 0, "d": 1}

JOBS = {
    "k0": (("near", "a"),),
    "k1": (("near", "b"), ("next", "a"), ("next", "b")),
    "k2": (("near", "c"), ("next", "c"), ("mid", "a"), ("mid", "b"), ("mid", "c")),
    "k3": (("near", "d"), ("next", "d"), ("mid", "d")),
    "k4": (("last", "a"), ("last", "b"), ("last", "c"), ("last", "d")),
}


def index(zl, x, zh, y, c):
    return (((zl * 4 + x) * 2 + zh) * 4 + y) * 2 + c


def pairs(dx, dy, dz, dc):
    out = []
    for zl in range(4):
        for x in range(4):
            for zh in range(2):
                for y in range(4):
                    for c in range(2):
                        z = (zh * 4 + zl + dz) % 8
                        src = index(z % 4, (x + dx) % 4, z // 4, (y + dy) % 4, (c + dc) % 2)
                        out.append((src, index(zl, x, zh, y, c)))
    return out


def take(v, dx=0, dy=0, dz=0, dc=0):
    return lax.ppermute(v, AXES, pairs(dx, dy, dz, dc))


def pack_kernel(s_ref, l_ref, o_ref):
    o_ref[:, :W] = s_ref[...]
    o_ref[:, W:] = l_ref[...].astype(F32)


def halves(x):
    hi = x.astype(BF16)
    return hi, (x - hi.astype(F32)).astype(BF16)


def spread_norm(x):
    n = jnp.sum(x * x, axis=1, keepdims=True) * (0.5 / W)
    return jnp.broadcast_to(n, (BLK, 128))


class Rows:
    def __init__(self, name):
        self.tiles = ROWS[name]
        self.blocks = 2 * len(self.tiles)
        n = self.blocks * BLK
        self.shapes = [((n, 2 * W + PERMS), BF16), ((n, 128), F32)]
        self.sums = [((n, PERMS), F32)]

    def fill(self, refs, raw):
        for i, ref in enumerate(raw):
            rows = slice(i * BLK, (i + 1) * BLK)
            x = ref[:, :W]
            hi, lo = halves(x * (1.0 / W))
            refs[0][rows, :W] = hi
            refs[0][rows, W : 2 * W] = lo
            refs[0][rows, 2 * W :] = ref[:, W:].astype(BF16)
            refs[1][rows, :] = spread_norm(x)


class Columns:
    def __init__(self, name):
        self.blocks = len(COLUMNS[name])
        self.width = self.blocks * BLK
        self.own = SELF[name] * BLK
        self.diag = COLUMNS[name][0] == (0, 0)
        self.shapes = [((self.width, 2 * W + PERMS), BF16), ((8, self.width), F32)]
        self.sums = [((8, self.width), F32)] * 2

    def fill(self, refs, raw):
        for j, ref in enumerate(raw):
            rows = slice(j * BLK, (j + 1) * BLK)
            x = ref[:, :W]
            hi, lo = halves(x)
            refs[0][rows, :W] = lo
            refs[0][rows, W : 2 * W] = hi
            refs[0][rows, 2 * W :] = ref[:, W:].astype(BF16)
            refs[1][:, rows] = spread_norm(x).T[:8, :]


def first_use(name):
    return next(job for job, work in JOBS.items() if any(name in pair for pair in work))


def sets_of(job):
    rows = list(dict.fromkeys(r for r, _ in JOBS[job]))
    cols = list(dict.fromkeys(c for _, c in JOBS[job]))
    return rows, cols


def sum_rows(job):
    at, start = {}, 0
    rows, cols = sets_of(job)
    for name in (*rows, *cols):
        at[name] = start
        start += Rows(name).blocks if name in ROWS else Columns(name).blocks
    return {**at, "end": start}


def dot_nt(a, b):
    return lax.dot_general(a, b, (((1,), (1,)), ((), ())), preferred_element_type=F32)


def side_by_side(a, width):
    return jnp.concatenate([a] * (width // 128), axis=1)


def piece(rows, r, cols, c, first, count, acc, wc, tt):
    dz = rows.tiles[first]
    lanes = slice(0 if dz <= 4 else cols.own, cols.width)
    width = lanes.stop - lanes.start
    at = slice(first * 256, (first + count) * 256)
    s = dot_nt(r[0][at, : 2 * W], c[0][lanes, : 2 * W]) + dot_nt(r[0][at, :W], c[0][lanes, W : 2 * W])
    s = (s - side_by_side(r[1][at, :], width)) - c[1][0:1, lanes]
    k = jnp.exp(jnp.minimum(s, 0.0))
    if dz in (0, 4) and cols.own == width:
        k = k * 0.5
    elif dz in (0, 4) and cols.own:
        lane = lax.broadcasted_iota(jnp.int32, (1, width), 1)
        k = k * jnp.where(lane < cols.own, 0.5, 1.0)
    if dz == 0 and cols.diag:
        i = lax.broadcasted_iota(jnp.int32, (BLK, BLK), 0)
        j = lax.broadcasted_iota(jnp.int32, (BLK, BLK), 1)
        top = jnp.concatenate([jnp.where(i == j, 0.0, k[:BLK, :BLK]), k[:BLK, BLK:]], axis=1)
        k = jnp.concatenate([top, k[BLK:, :]], axis=0)
    hi, lo = halves(k)
    lab = c[0][lanes, 2 * W :]
    acc[at, :] += jnp.dot(hi, lab, preferred_element_type=F32) + jnp.dot(lo, lab, preferred_element_type=F32)
    observed = jnp.broadcast_to(r[0][at, 2 * W : 2 * W + 1].astype(F32), (count * 256, 128))
    wc[0:1, lanes] += jnp.sum(k * side_by_side(observed, width), axis=0, keepdims=True)
    tt[0:1, lanes] += jnp.sum(k, axis=0, keepdims=True)


def groups(rows, cols):
    out = []
    for t, dz in enumerate(rows.tiles):
        kind = 1 if not cols.own else 0 if dz in (0, 4) else 1 if dz < 4 else 2
        if kind == 2 and cols.own == cols.width:
            continue
        if out and out[-1][2] == kind and out[-1][0] + out[-1][1] == t and out[-1][1] < 2:
            out[-1][1] += 1
        else:
            out.append([t, 1, kind])
    return [(first, count) for first, count, _ in out]


def clear(*refs):
    for ref in refs:
        ref[...] = jnp.zeros_like(ref)


def job_kernel(job, raw_counts, ready_names, made_names, tail, *refs):
    rows, cols = sets_of(job)
    shape_of = {name: Rows(name) if name in ROWS else Columns(name) for name in (*rows, *cols)}
    refs = list(refs)

    def pop(n):
        head, refs[:] = refs[:n], refs[n:]
        return head

    raw = {name: pop(n) for name, n in raw_counts}
    ready = {name: pop(2) for name in ready_names}
    before = pop(tail)
    out = pop(1)[0]
    kept = pop(1)[0] if tail else None
    made = {name: pop(2) for name in made_names}
    for name, _ in raw_counts:
        ready[name] = made[name] if name in made else pop(2)
        shape_of[name].fill(ready[name], raw[name])
    acc = {name: pop(1)[0] for name in rows}
    sums = {name: pop(2) for name in cols}
    if tail:
        sent, out = out, pop(1)[0]
    clear(*acc.values(), *(ref for pair in sums.values() for ref in pair))
    for r, c in JOBS[job]:
        for first, count in groups(shape_of[r], shape_of[c]):
            piece(shape_of[r], ready[r], shape_of[c], ready[c], first, count, acc[r], *sums[c])
    at = sum_rows(job)
    quad = jnp.zeros((1, PERMS), F32)
    for name in rows:
        for i in range(shape_of[name].blocks):
            here = slice(i * BLK, (i + 1) * BLK)
            part = acc[name][here, :]
            quad = quad + jnp.sum(part * ready[name][0][here, 2 * W :].astype(F32), axis=0, keepdims=True)
            out[at[name] + i : at[name] + i + 1, :] = part[:, :128].T[0:1, :]
    tot = jnp.zeros((1, 128), F32)
    for name in cols:
        wc, tt = sums[name]
        for j in range(shape_of[name].blocks):
            lanes = slice(j * BLK, (j + 1) * BLK)
            out[at[name] + j : at[name] + j + 1, :] = wc[0:1, lanes]
            tot = tot + tt[0:1, lanes]
    end = at["end"]
    out[end : end + 1, :] = quad[:, :128]
    out[end + 1 : end + 2, :] = quad[:, 128:]
    out[end + 2 : end + 3, :] = tot
    if tail:
        send_sums(tuple(zip(JOBS, [*before, out])), sent, kept)


def send_sums(parts, sent, kept):
    def row_of(name, i):
        found = [(ref, sum_rows(job)) for job, ref in parts]
        rows = [ref[at[name] + i : at[name] + i + 1, :] for ref, at in found if name in at]
        return functools.reduce(jnp.add, rows)

    all_rows = 256 * BLK
    half = all_rows / 2.0
    pair = 2.0 * half * (half - 1.0)
    total = jnp.sum(row_of("end", 2))
    for k in range(2):
        share = (2.0 / pair) * total + (2.0 * (2.0 * half - 1.0) / pair) * row_of("end", k)
        sent[:, (1 + k) * BLK : (2 + k) * BLK] = jnp.broadcast_to(share, (16, BLK))
    zl, x, zh, y, c = (lax.axis_index(a) for a in AXES)
    z = zh * 4 + zl
    device = lax.broadcasted_iota(jnp.int32, (16, BLK), 0)
    line = jnp.zeros((16, BLK), F32)
    for name, tiles in ROWS.items():
        for i, dz in enumerate(tiles):
            for side in range(2):
                pz = (z + dz) % 8
                peer = (pz % 4 * 2 + pz // 4) * 2 + (c + side) % 2
                line = jnp.where(device == peer, row_of(name, 2 * i + side), line)
    sent[:, :BLK] = line
    plane = jnp.zeros((16, BLK), F32)
    for name, offsets in COLUMNS.items():
        for i, (dx, dy) in enumerate(offsets):
            peer = (x + dx) % 4 * 4 + (y + dy) % 4
            plane = jnp.where(device == peer, row_of(name, i), plane)
    kept[...] = plane


def kernel_between(got, kept, sent):
    both = jnp.sum(got[...], axis=0)
    me = lax.axis_index("x") * 4 + lax.axis_index("y")
    device = lax.broadcasted_iota(jnp.int32, (16, BLK), 0)
    sent[:, :BLK] = kept[...] + jnp.where(device == me, both[:, :BLK], 0.0)
    sent[:, BLK:] = jnp.broadcast_to(both[:, BLK:], (16, PERMS))


def kernel_end(all_rows, got, statistic, proof, p_value):
    both = jnp.sum(got[...], axis=0)
    proof[...] = both[:, :BLK] / jnp.sqrt(jnp.full((1, BLK), all_rows, F32))
    s = both[:, BLK:]
    statistic[...] = s
    part = jax.nn.sigmoid(4.0 * (s - s[:, 0:1]))
    lane = lax.broadcasted_iota(jnp.int32, (1, PERMS), 1)
    p_value[...] = jnp.sum(jnp.where(lane > 0, part, 0.0), axis=1, keepdims=True) / (PERMS - 1.0)


def run(job, raw, ready, before=None):
    rows, cols = sets_of(job)
    names = [name for name in (*rows, *cols) if first_use(name) == job]
    reused = [name for name in (*rows, *cols) if first_use(name) != job]
    shape_of = {name: Rows(name) if name in ROWS else Columns(name) for name in (*rows, *cols)}
    made = [] if before else names
    ins = [b for name in names for b in raw[name]] + [a for name in reused for a in ready[name]] + (before or [])
    n_out = -(-(sum_rows(job)["end"] + 3) // 8) * 8
    outs = [((16, BLK + PERMS), F32), ((16, BLK), F32)] if before else [((n_out, 128), F32)]
    outs += [s for name in made for s in shape_of[name].shapes]
    scratch = [s for name in names if name not in made for s in shape_of[name].shapes]
    scratch += [s for name in (*rows, *cols) for s in shape_of[name].sums]
    if before:
        scratch.append(((n_out, 128), F32))
    cells = sum(Rows(r).blocks * Columns(c).blocks for r, c in JOBS[job]) * BLK * BLK
    vmem = pl.BlockSpec(memory_space=pltpu.VMEM)
    out, *bundles = pl.pallas_call(
        functools.partial(job_kernel, job, [(name, len(raw[name])) for name in names], reused, made, len(before or [])),
        out_shape=[jax.ShapeDtypeStruct(*s) for s in outs],
        in_specs=[vmem] * len(ins),
        out_specs=[vmem] * len(outs),
        scratch_shapes=[pltpu.VMEM(*s) for s in scratch],
        cost_estimate=pl.CostEstimate(
            flops=cells * 2 * (3 * W + 2 * PERMS), bytes_accessed=8 << 20, transcendentals=cells
        ),
        compiler_params=pltpu.CompilerParams(vmem_limit_bytes=8 << 20),
    )(*ins)
    for k, name in enumerate(made):
        ready[name] = bundles[2 * k : 2 * k + 2]
    return (out, *bundles) if before else out


def shards(samples, labels):
    vmem = pl.BlockSpec(memory_space=pltpu.VMEM)
    all_rows = samples.shape[0] * 256
    own = pl.pallas_call(
        pack_kernel,
        out_shape=jax.ShapeDtypeStruct((BLK, COLS), F32),
        in_specs=[vmem, vmem],
        out_specs=vmem,
        compiler_params=pltpu.CompilerParams(vmem_limit_bytes=4 << 20),
        name="pack",
    )(samples, labels)
    u1 = take(own, dz=1)
    d1 = take(own, dz=-1)
    c10 = take(own, dx=1)
    c03 = take(own, dy=-1)
    c20 = take(c10, dx=1)
    c02 = take(c03, dy=-1)
    u2 = take(u1, dz=1)
    d2 = take(d1, dz=-1)
    c32 = take(c02, dx=-1)
    c22 = take(c32, dx=-1)
    c21 = take(c20, dy=1)
    c11 = take(c10, dy=1)
    c13 = take(c10, dy=-1)
    u3 = take(u2, dz=1)
    d3 = take(d2, dz=-1)
    u4 = take(u3, dz=1)
    line = {0: own, 1: u1, 2: u2, 3: u3, 4: u4, 5: d3, 6: d2, 7: d1}
    rows = {dz: (b, take(b, dc=1)) for dz, b in line.items()}

    plane = {
        **{(0, 0): own, (1, 0): c10, (0, 3): c03, (2, 0): c20, (0, 2): c02},
        **{(1, 1): c11, (1, 3): c13, (3, 2): c32, (2, 1): c21, (2, 2): c22},
    }
    raw = {name: [b for dz in tiles for b in rows[dz]] for name, tiles in ROWS.items()}
    raw |= {name: [plane[at] for at in offsets] for name, offsets in COLUMNS.items()}
    ready, before = {}, []
    for job in list(JOBS)[:-1]:
        before.append(run(job, raw, ready))
    sent, kept = run(list(JOBS)[-1], raw, ready, before)

    def exchange(v, axes):
        return lax.all_to_all(v.reshape(16, 1, COLS // 2), axes, 0, 0, tiled=True)

    got = exchange(sent, ("zl", "zh", "c"))
    sent = pl.pallas_call(
        kernel_between,
        out_shape=jax.ShapeDtypeStruct((16, COLS // 2), F32),
        in_specs=[vmem] * 2,
        out_specs=vmem,
        compiler_params=pltpu.CompilerParams(vmem_limit_bytes=8 << 20),
        name="between",
    )(got, kept)
    got = exchange(sent, ("x", "y"))
    statistic, proof, p_value = pl.pallas_call(
        functools.partial(kernel_end, float(all_rows)),
        out_shape=[jax.ShapeDtypeStruct((1, n), F32) for n in (PERMS, BLK, 1)],
        in_specs=[vmem],
        out_specs=[vmem] * 3,
        compiler_params=pltpu.CompilerParams(vmem_limit_bytes=8 << 20),
        name="end",
    )(got)
    return (statistic.reshape(PERMS), proof.reshape(BLK), p_value.reshape(()))


def solution(mesh):
    torus = Mesh(mesh.devices.reshape(SIZES), AXES)
    return jax.shard_map(
        shards,
        mesh=torus,
        in_specs=(P(AXES, None), P(AXES, None)),
        out_specs=(P(), P(AXES), P()),
        check_vma=False,
    )
```
